16 devices in a mesh: data: 16 (over z, y, x, core).
Axes of the slice: x: 2, y: 2, z: 2, core: 2. Of those that a mesh axis runs over, the one named last changes fastest.
Arguments:
- inputs: bfloat16 [256, 8, 1152], P('data')
- out_grad: float32 [256, 8, 1152], P('data')
- w_fwd0: bfloat16 [2304, 4608], replicated
- b_fwd0: float32 [4608], replicated
- w_rev0: bfloat16 [2304, 4608], replicated
- b_rev0: float32 [4608], replicated
- w_upper: bfloat16 [2, 2304, 4608], replicated
- b_upper: float32 [2, 4608], replicated
Outputs:
- output 1: float32 [256, 8, 1152], P('data')
- output 2: float32 [2304, 4608], replicated
- output 3: float32 [4608], replicated
- output 4: float32 [2304, 4608], replicated
- output 5: float32 [4608], replicated
- output 6: float32 [2, 2304, 4608], replicated
- output 7: float32 [2, 4608], replicated
All inputs are finite; a program needn't handle non-finite values.
Results may differ from the reference program's by a relative error of at most 0.0139591.
Values are sent between devices in bfloat16 or wider.
A program may use at most 1 GiB of HBM per device.

```python
import jax
import jax.numpy as jnp
from jax import lax

HIDDEN = 1152
LAYERS = 3
SEQ = 8
BATCH_DEV = 16
GROUPS = 16

BATCH = BATCH_DEV * GROUPS


def setup_inputs(seed: int = 0) -> dict:
    key_list = jax.random.split(jax.random.key(seed), 8)
    w_scale = HIDDEN ** -0.5
    forget_shift = jnp.concatenate([jnp.zeros((HIDDEN,), jnp.float32), jnp.ones((HIDDEN,), jnp.float32), jnp.zeros((2 * HIDDEN,), jnp.float32)])
    act_shape = (BATCH, SEQ, HIDDEN)
    cat_shape = (2 * HIDDEN, 4 * HIDDEN)
    inputs = jax.random.normal(key_list[0], act_shape, jnp.float32).astype(jnp.bfloat16)
    out_grad = jax.random.normal(key_list[1], act_shape, jnp.float32)
    w_fwd0 = (jax.random.normal(key_list[2], cat_shape, jnp.float32) * w_scale).astype(jnp.bfloat16)
    b_fwd0 = 0.5 * jax.random.normal(key_list[3], (4 * HIDDEN,), jnp.float32) + forget_shift
    w_rev0 = (jax.random.normal(key_list[4], cat_shape, jnp.float32) * w_scale).astype(jnp.bfloat16)
    b_rev0 = 0.5 * jax.random.normal(key_list[5], (4 * HIDDEN,), jnp.float32) + forget_shift
    w_upper = (jax.random.normal(key_list[6], (LAYERS - 1,) + cat_shape, jnp.float32) * w_scale).astype(jnp.bfloat16)
    b_upper = 0.5 * jax.random.normal(key_list[7], (LAYERS - 1, 4 * HIDDEN), jnp.float32) + forget_shift
    return dict(inputs=inputs, out_grad=out_grad, w_fwd0=w_fwd0, b_fwd0=b_fwd0, w_rev0=w_rev0, b_rev0=b_rev0, w_upper=w_upper, b_upper=b_upper)


def cell_forward(pre_seq, w_rec, bias_vec, backwards):
    hidden_size = w_rec.shape[0]

    def cell_step(carry_in, pre_t):
        h_prev, c_prev = carry_in
        z_all = pre_t + jnp.dot(h_prev, w_rec, preferred_element_type=jnp.float32) + bias_vec
        in_gate = jax.nn.sigmoid(z_all[:, :hidden_size])
        forget_gate = jax.nn.sigmoid(z_all[:, hidden_size:2 * hidden_size])
        cand_gate = jnp.tanh(z_all[:, 2 * hidden_size:3 * hidden_size])
        out_gate = jax.nn.sigmoid(z_all[:, 3 * hidden_size:])
        c_new = forget_gate * c_prev + in_gate * cand_gate
        h_new = out_gate * jnp.tanh(c_new)
        gate_all = jnp.concatenate([in_gate, forget_gate, cand_gate, out_gate], axis=-1)
        return (h_new.astype(jnp.bfloat16), c_new), (gate_all, c_prev, h_new)

    batch_rows = pre_seq.shape[1]
    init_carry = (jnp.zeros((batch_rows, hidden_size), jnp.bfloat16), jnp.zeros((batch_rows, hidden_size), jnp.float32))
    return lax.scan(cell_step, init_carry, pre_seq, reverse=backwards)[1]


def cell_backward(dh_seq, gate_seq, c_prevs, w_rec, backwards):
    hidden_size = w_rec.shape[0]

    def back_step(carry_in, step_in):
        dh_rec, dc_next, db_rows = carry_in
        dh_in, gate_all, c_prev = step_in
        in_gate = gate_all[:, :hidden_size]
        forget_gate = gate_all[:, hidden_size:2 * hidden_size]
        cand_gate = gate_all[:, 2 * hidden_size:3 * hidden_size]
        out_gate = gate_all[:, 3 * hidden_size:]
        tanh_c = jnp.tanh(forget_gate * c_prev + in_gate * cand_gate)
        dh_tot = dh_in + dh_rec
        dc_cur = dc_next + dh_tot * out_gate * (1.0 - tanh_c * tanh_c)
        dz_all = jnp.concatenate([
            dc_cur * cand_gate * in_gate * (1.0 - in_gate),
            dc_cur * c_prev * forget_gate * (1.0 - forget_gate),
            dc_cur * in_gate * (1.0 - cand_gate * cand_gate),
            dh_tot * tanh_c * out_gate * (1.0 - out_gate)], axis=-1)
        dz_bf = dz_all.astype(jnp.bfloat16)
        dh_back = jnp.dot(dz_bf, w_rec.T, preferred_element_type=jnp.float32)
        return (dh_back, dc_cur * forget_gate, db_rows + dz_all), dz_bf

    batch_rows = dh_seq.shape[1]
    init_carry = (jnp.zeros((batch_rows, hidden_size), jnp.float32), jnp.zeros((batch_rows, hidden_size), jnp.float32), jnp.zeros((batch_rows, 4 * hidden_size), jnp.float32))
    final_carry, dz_seq = lax.scan(back_step, init_carry, (dh_seq, gate_seq, c_prevs), reverse=not backwards)
    return dz_seq, jnp.sum(final_carry[2], axis=0)


def weight_grads(layer_x, x_form, h_bf, dz_seq, backwards):
    dz_wide = dz_seq.astype(jnp.float32)
    h_wide = h_bf.astype(jnp.float32)
    x_part = jnp.einsum(x_form, layer_x.astype(jnp.float32), dz_wide)
    if backwards:
        h_part = jnp.einsum('tbh,tbg->hg', h_wide[1:], dz_wide[:-1])
    else:
        h_part = jnp.einsum('tbh,tbg->hg', h_wide[:-1], dz_wide[1:])
    return jnp.concatenate([x_part, h_part], axis=0)


def layer_forward(layer_x, x_form, w_cat, bias_vec, backwards):
    hidden_size = w_cat.shape[0] // 2
    pre_seq = jnp.einsum(x_form, layer_x.astype(jnp.float32), w_cat[:hidden_size].astype(jnp.float32))
    return cell_forward(pre_seq, w_cat[hidden_size:], bias_vec, backwards)


def block_grads(inputs, out_grad, w_fwd0, b_fwd0, w_rev0, b_rev0, w_upper, b_upper):
    gate_f, cprev_f, hseq_f = layer_forward(inputs, 'bth,hg->tbg', w_fwd0, b_fwd0, False)
    gate_r, cprev_r, hseq_r = layer_forward(inputs, 'bth,hg->tbg', w_rev0, b_rev0, True)
    first_out = (hseq_f + hseq_r).astype(jnp.bfloat16)

    def up_forward(layer_x, layer_par):
        w_cat, bias_vec = layer_par
        gate_seq, c_prevs, h_seq = layer_forward(layer_x, 'tbh,hg->tbg', w_cat, bias_vec, False)
        h_bf = h_seq.astype(jnp.bfloat16)
        return h_bf, (layer_x, gate_seq, c_prevs, h_bf)

    saved = lax.scan(up_forward, first_out, (w_upper, b_upper))[1]

    def up_backward(dh_seq, layer_par):
        w_cat, layer_saved = layer_par
        layer_x, gate_seq, c_prevs, h_bf = layer_saved
        hidden_size = w_cat.shape[0] // 2
        dz_seq, db_sum = cell_backward(dh_seq, gate_seq, c_prevs, w_cat[hidden_size:], False)
        dw_cat = weight_grads(layer_x, 'tbh,tbg->hg', h_bf, dz_seq, False)
        dh_below = jnp.einsum('tbg,hg->tbh', dz_seq.astype(jnp.float32), w_cat[:hidden_size].astype(jnp.float32))
        return dh_below, (dw_cat, db_sum)

    dh_first, up_grads = lax.scan(up_backward, jnp.swapaxes(out_grad, 0, 1), (w_upper, saved), reverse=True)
    dz_f, db_fwd0 = cell_backward(dh_first, gate_f, cprev_f, w_fwd0[HIDDEN:], False)
    dz_r, db_rev0 = cell_backward(dh_first, gate_r, cprev_r, w_rev0[HIDDEN:], True)
    dw_fwd0 = weight_grads(inputs, 'bth,tbg->hg', hseq_f.astype(jnp.bfloat16), dz_f, False)
    dw_rev0 = weight_grads(inputs, 'bth,tbg->hg', hseq_r.astype(jnp.bfloat16), dz_r, True)
    in_grad = jnp.einsum('tbg,hg->bth', dz_f.astype(jnp.float32), w_fwd0[:HIDDEN].astype(jnp.float32)) + jnp.einsum('tbg,hg->bth', dz_r.astype(jnp.float32), w_rev0[:HIDDEN].astype(jnp.float32))
    return in_grad, dw_fwd0, db_fwd0, dw_rev0, db_rev0, up_grads[0], up_grads[1]


def reference(inputs, out_grad, w_fwd0, b_fwd0, w_rev0, b_rev0, w_upper, b_upper):
    in_blocks = inputs.reshape(GROUPS, BATCH_DEV, SEQ, HIDDEN)
    grad_blocks = out_grad.reshape(GROUPS, BATCH_DEV, SEQ, HIDDEN)

    def accumulate(run_sums, block_pair):
        block_out = block_grads(block_pair[0], block_pair[1], w_fwd0, b_fwd0, w_rev0, b_rev0, w_upper, b_upper)
        new_sums = tuple(run_sum + block_sum for run_sum, block_sum in zip(run_sums, block_out[1:]))
        return new_sums, block_out[0]

    zero_sums = (
        jnp.zeros((2 * HIDDEN, 4 * HIDDEN), jnp.float32),
        jnp.zeros((4 * HIDDEN,), jnp.float32),
        jnp.zeros((2 * HIDDEN, 4 * HIDDEN), jnp.float32),
        jnp.zeros((4 * HIDDEN,), jnp.float32),
        jnp.zeros((LAYERS - 1, 2 * HIDDEN, 4 * HIDDEN), jnp.float32),
        jnp.zeros((LAYERS - 1, 4 * HIDDEN), jnp.float32))
    grad_sums, in_grads = lax.scan(accumulate, zero_sums, (in_blocks, grad_blocks))
    in_grad = in_grads.reshape(BATCH, SEQ, HIDDEN)
    return (in_grad, grad_sums[0], grad_sums[1], grad_sums[2], grad_sums[3], grad_sums[4], grad_sums[5])
```

```python
import functools

import jax
import jax.numpy as jnp
from jax import lax
from jax.experimental import pallas as pl
from jax.experimental.pallas import tpu as pltpu
from jax.sharding import PartitionSpec as P

DATA_AXIS = 'data'
F32 = jnp.float32
BF16 = jnp.bfloat16
VMEM_LIMIT = 60 * 1024 * 1024


def dot_nt(lhs, rhs):
    return lax.dot_general(lhs, rhs, (((1,), (1,)), ((), ())), preferred_element_type=F32)


class Exchange:
    def __init__(self, ref, sems):
        self.ref, self.sems = ref, sems
        self.third = ref.shape[2] // 3
        self.me = lax.axis_index(DATA_AXIS)
        self.started = []

    def flip(self, dev, bit):
        return dev + bit * (1 - 2 * ((dev // bit) % 2))

    def bits(self, part):
        return [2 << ((part + r) % 3) for r in range(3)]

    def copies(self, part, rnd):
        bits = self.bits(part)
        peer = self.flip(self.me, bits[rnd])
        out = []
        for j in range(1 << rnd):
            blk, got = self.me, peer
            for k in range(rnd):
                if (j >> k) & 1:
                    blk, got = self.flip(blk, bits[k]), self.flip(got, bits[k])
            out.append((blk, got, peer, part * 7 + (1 << rnd) - 1 + j))
        return out

    def remote(self, blk, cols, peer, slot):
        view = self.ref.at[blk, :, cols]
        return pltpu.make_async_remote_copy(
            src_ref=view, dst_ref=view, send_sem=self.sems.at[0, slot], recv_sem=self.sems.at[1, slot],
            device_id=(peer,), device_id_type=pl.DeviceIdType.MESH)

    def cols(self, part):
        return pl.ds(part * self.third, self.third)

    def each(self, rnd):
        for part in range(3):
            for blk, got, peer, slot in self.copies(part, rnd):
                yield part, blk, got, peer, slot

    def send(self, rnd):
        for part, blk, got, peer, slot in self.each(rnd):
            self.remote(blk, self.cols(part), peer, slot).start()

    def wait(self, rnd):
        for part, blk, got, peer, slot in self.each(rnd):
            self.remote(blk, self.cols(part), peer, slot).wait()

    def own(self):
        return self.remote(self.me, pl.ds(0, 3 * self.third), self.flip(self.me, 1), 21)

    def share(self, rnd, start):
        for part, blk, got, peer, slot in self.each(rnd):
            copy = self.remote(got, self.cols(part), self.flip(self.me, 1), 22 + slot)
            if start:
                copy.start()
            else:
                copy.wait()


SLOTS = 43


def run_stage(ex, stage, open_ops):
    if stage > 0:
        if ('round', stage - 1) in open_ops:
            ex.wait(stage - 1)
            open_ops.remove(('round', stage - 1))
        ex.share(stage - 1, True)
        open_ops.append(('share', stage - 1))
    else:
        ex.own().start()
        open_ops.append(('own', 0))
    if stage < 3:
        ex.send(stage)
        open_ops.append(('round', stage))


class Comm:
    def __init__(self, plan, refs, sems, local_sems, sources):
        self.plan = plan
        self.exs = [Exchange(ref, sems.at[n]) for n, ref in enumerate(refs)]
        self.open_ops = [[] for _ in plan]
        self.local = [None if src is None else pltpu.make_async_copy(src, ex.ref.at[ex.me], local_sems.at[n])
                      for n, (src, ex) in enumerate(zip(sources, self.exs))]

    def begin(self):
        if not self.plan:
            return
        for copy in self.local:
            if copy is not None:
                copy.start()
        barrier = pltpu.get_barrier_semaphore()
        ex = self.exs[0]
        for bit in (1, 2, 4, 8):
            pl.semaphore_signal(barrier, inc=1, device_id=(ex.flip(ex.me, bit),),
                                device_id_type=pl.DeviceIdType.MESH)
        pl.semaphore_wait(barrier, 4)
        for copy in self.local:
            if copy is not None:
                copy.wait()
        self.at('start')

    def at(self, point):
        for ex, plan, ops in zip(self.exs, self.plan, self.open_ops):
            for stage in plan.get(point, ()):
                run_stage(ex, stage, ops)

    def in_loop(self, idx):
        points = sorted({p for plan in self.plan for p in plan if isinstance(p, int)})
        for point in points:
            pl.when(idx == point)(functools.partial(self.at, point))

    def finish(self):
        self.at('end')
        for ex, ops in zip(self.exs, self.open_ops):
            for kind, rnd in ops:
                if kind == 'round':
                    ex.wait(rnd)
                elif kind == 'share':
                    ex.share(rnd, False)
                else:
                    ex.own().wait()


def fwd_kernel(layer, steps, backwards, with_sum, plan, sources, *refs):
    refs = list(refs)
    x_ref, w_hbm, b_ref = refs[:3]
    refs = refs[3:]
    other_ref = refs.pop(0) if with_sum else None
    srcs = [x_ref if s == 'x' else refs.pop(0) if s == 'arg' else None for s in sources]
    refs = refs[sum(s == 'alias' for s in sources):]
    gate_ref, cprev_ref, h_ref, hbf_ref = refs[:4]
    refs = refs[4:]
    sum_ref = refs.pop(0) if with_sum else None
    g_refs = [refs.pop(0) for _ in plan]
    w_buf, pre, sems = refs[:3]
    comm = Comm(plan, g_refs, *(refs[3:5] if plan else (None, None)), srcs)
    hid = x_ref.shape[1]
    rows = x_ref.shape[0] // steps
    w_src = w_hbm if layer is None else w_hbm.at[layer]

    def w_copy(part, gate):
        at = (pl.ds(part * hid, hid), pl.ds(gate * hid, hid))
        return pltpu.make_async_copy(w_src.at[at], w_buf.at[at], sems.at[part * 4 + gate])

    for part in range(2):
        for gate in range(4):
            w_copy(part, gate).start()
    comm.begin()
    for gate in range(4):
        w_copy(0, gate).wait()
        cols = pl.ds(gate * hid, hid)
        pre[:, cols] = jnp.dot(x_ref[...], w_buf[:hid, cols], preferred_element_type=F32) + b_ref[:, cols]

    def cell(t, z_all, c_prev):
        in_gate = jax.nn.sigmoid(z_all[:, :hid])
        forget_gate = jax.nn.sigmoid(z_all[:, hid:2 * hid])
        cand_gate = jnp.tanh(z_all[:, 2 * hid:3 * hid])
        out_gate = jax.nn.sigmoid(z_all[:, 3 * hid:])
        c_new = forget_gate * c_prev + in_gate * cand_gate
        h_new = out_gate * jnp.tanh(c_new)
        gate_ref[t, :, :hid] = in_gate
        gate_ref[t, :, hid:2 * hid] = forget_gate
        gate_ref[t, :, 2 * hid:3 * hid] = cand_gate
        gate_ref[t, :, 3 * hid:] = out_gate
        cprev_ref[t] = c_prev
        h_ref[t] = h_new
        h_bf = h_new.astype(BF16)
        at = pl.ds(t * rows, rows) if isinstance(t, int) else pl.ds(pl.multiple_of(t * rows, rows), rows)
        hbf_ref[at, :] = h_bf
        if with_sum:
            sum_ref[at, :] = (other_ref[t] + h_new).astype(BF16)
        return h_bf, c_new

    first = steps - 1 if backwards else 0
    carry = cell(first, pre[first * rows:(first + 1) * rows, :], jnp.zeros((rows, hid), F32))
    for gate in range(4):
        w_copy(1, gate).wait()

    def step(idx, carry):
        h_bf, c_prev = carry
        comm.in_loop(idx)
        t = steps - 1 - idx if backwards else idx
        z_all = pre[pl.ds(pl.multiple_of(t * rows, rows), rows), :] + jnp.dot(
            h_bf, w_buf[hid:, :], preferred_element_type=F32)
        return cell(t, z_all, c_prev)

    lax.fori_loop(1, steps, step, carry)
    comm.finish()


def call(kernel, name, args, n_vmem, outs, scratch, plan, blocks, aliases, collective, flops):
    vm, hbm = pl.BlockSpec(memory_space=pltpu.VMEM), pl.BlockSpec(memory_space=pl.ANY)
    in_specs = [hbm if n == 1 or n >= n_vmem else vm for n in range(len(args))]
    out_specs = [vm] * len(outs) + [hbm] * len(blocks)
    params = dict(vmem_limit_bytes=VMEM_LIMIT)
    if plan:
        params.update(collective_id=collective, has_side_effects=True)
        scratch = scratch + [pltpu.SemaphoreType.DMA((len(plan), 2, SLOTS)), pltpu.SemaphoreType.DMA((len(plan),))]
    return pl.pallas_call(
        kernel,
        out_shape=outs + [jax.ShapeDtypeStruct(shape, BF16) for shape in blocks],
        in_specs=in_specs,
        out_specs=out_specs,
        scratch_shapes=scratch,
        input_output_aliases=aliases,
        compiler_params=pltpu.CompilerParams(**params),
        cost_estimate=pl.CostEstimate(flops=flops, bytes_accessed=40 << 20, transcendentals=0),
        name=name,
    )(*args)


def gather_args(args, gathers, n_outs, x_rows):
    args += [blk for kind, blk, _ in gathers if kind == 'arg']
    n_vmem = len(args)
    aliases = {}
    blocks = []
    devs = lax.axis_size(DATA_AXIS)
    for n, (kind, blk, _) in enumerate(gathers):
        if kind == 'alias':
            aliases[len(args)] = n_outs + n
            args.append(blk)
            blocks.append(blk.shape)
        else:
            blocks.append((devs,) + (x_rows if kind == 'x' else blk).shape)
    return [p for _, _, p in gathers], [kind for kind, _, _ in gathers], blocks, n_vmem, aliases


def lstm_forward(x_rows, w_cat, layer, bias_row, steps, backwards, collective, other=None, gathers=()):
    hid = x_rows.shape[1]
    rows = x_rows.shape[0] // steps
    with_sum = other is not None
    outs = [jax.ShapeDtypeStruct((steps, rows, 4 * hid), F32),
            jax.ShapeDtypeStruct((steps, rows, hid), F32),
            jax.ShapeDtypeStruct((steps, rows, hid), F32),
            jax.ShapeDtypeStruct((steps * rows, hid), BF16)]
    args = [x_rows, w_cat, bias_row]
    if with_sum:
        outs.append(jax.ShapeDtypeStruct((steps * rows, hid), BF16))
        args.append(other)
    plan, sources, blocks, n_vmem, aliases = gather_args(args, gathers, len(outs), x_rows)
    return call(functools.partial(fwd_kernel, layer, steps, backwards, with_sum, plan, sources), 'lstm_fwd', args,
                n_vmem, outs,
                [pltpu.VMEM((2 * hid, 4 * hid), BF16), pltpu.VMEM((steps * rows, 4 * hid), F32),
                 pltpu.SemaphoreType.DMA((8,))],
                plan, blocks, aliases, collective, 4 * steps * rows * hid * 4 * hid * 8)


def bwd_kernel(layer, steps, backwards, with_sum, plan, sources, *refs):
    refs = list(refs)
    dh_ref, w_hbm, gate_ref, cprev_ref = refs[:4]
    refs = refs[4:]
    other_ref = refs.pop(0) if with_sum else None
    srcs = [refs.pop(0) if s == 'arg' else None for s in sources]
    refs = refs[sum(s == 'alias' for s in sources):]
    dz_ref, db_ref, dx_ref = refs[:3]
    refs = refs[3:]
    g_refs = [refs.pop(0) for _ in plan]
    w_buf, sems = refs[:2]
    comm = Comm(plan, g_refs, *(refs[2:4] if plan else (None, None)), srcs)
    rows, hid = dh_ref.shape[1:]
    w_src = w_hbm if layer is None else w_hbm.at[layer]

    def w_copy(part):
        at = pl.ds(part * hid, hid)
        return pltpu.make_async_copy(w_src.at[at], w_buf.at[at], sems.at[part])

    w_copy(1).start()
    w_copy(0).start()
    comm.begin()

    def cell(t, dh_rec, dc_next):
        in_gate = gate_ref[t, :, :hid]
        forget_gate = gate_ref[t, :, hid:2 * hid]
        cand_gate = gate_ref[t, :, 2 * hid:3 * hid]
        out_gate = gate_ref[t, :, 3 * hid:]
        c_prev = cprev_ref[t]
        tanh_c = jnp.tanh(forget_gate * c_prev + in_gate * cand_gate)
        dh_tot = dh_ref[t] + dh_rec
        dc_cur = dc_next + dh_tot * out_gate * (1.0 - tanh_c * tanh_c)
        parts = [dc_cur * cand_gate * in_gate * (1.0 - in_gate),
                 dc_cur * c_prev * forget_gate * (1.0 - forget_gate),
                 dc_cur * in_gate * (1.0 - cand_gate * cand_gate),
                 dh_tot * tanh_c * out_gate * (1.0 - out_gate)]
        at = pl.ds(pl.multiple_of(t * rows, rows), rows)
        for gate, part in enumerate(parts):
            cols = slice(gate * hid, (gate + 1) * hid)
            dz_ref[at, cols] = part.astype(BF16)
            db_ref[:, cols] += part[:8] + part[8:]
        return dc_cur * forget_gate

    db_ref[...] = jnp.zeros_like(db_ref)
    first = 0 if backwards else steps - 1
    zero = jnp.zeros((rows, hid), F32)
    dc = cell(first, zero, zero)
    w_copy(1).wait()

    def step(idx, dc_next):
        comm.in_loop(idx)
        prev = idx - 1 if backwards else steps - idx
        t = idx if backwards else steps - 1 - idx
        at = pl.ds(pl.multiple_of(prev * rows, rows), rows)
        dh_rec = dot_nt(dz_ref[at, :], w_buf[hid:, :])
        return cell(t, dh_rec, dc_next)

    lax.fori_loop(1, steps, step, dc)
    w_copy(0).wait()
    dx = dot_nt(dz_ref[...], w_buf[:hid, :])
    if with_sum:
        dx = dx + other_ref[...]
    dx_ref[...] = dx
    comm.finish()


def lstm_backward(dh_seq, w_cat, layer, gate_seq, c_prevs, backwards, collective, other=None, gathers=()):
    steps, rows, hid = dh_seq.shape
    with_sum = other is not None
    args = [dh_seq, w_cat, gate_seq, c_prevs] + ([other] if with_sum else [])
    plan, sources, blocks, n_vmem, aliases = gather_args(args, gathers, 3, None)
    return call(functools.partial(bwd_kernel, layer, steps, backwards, with_sum, plan, sources), 'lstm_bwd', args,
                n_vmem,
                [jax.ShapeDtypeStruct((steps * rows, 4 * hid), BF16),
                 jax.ShapeDtypeStruct((8, 4 * hid), F32),
                 jax.ShapeDtypeStruct((steps * rows, hid), F32)],
                [pltpu.VMEM((2 * hid, 4 * hid), BF16), pltpu.SemaphoreType.DMA((2,))],
                plan, blocks, aliases, collective, 4 * steps * rows * hid * 4 * hid * 12)


def dw_kernel(backwards, steps, rows, x_ref, h_ref, dz_ref, *refs):
    out_ref, shifted, turned = refs[-3:]
    part, col = pl.program_id(0), pl.program_id(1)
    span = steps * rows
    devs = x_ref.shape[0] // span

    def turn(src):
        for n in range(devs):
            at = slice(n * span, (n + 1) * span)
            turned[:, at] = src[at, :].T

    @pl.when((part == 0) & (col == 0))
    def _():
        turn(x_ref)

    @pl.when((part == 1) & (col == 0))
    def _():
        none = jnp.zeros((rows, h_ref.shape[1]), BF16)
        for n in range(devs):
            lo, hi = n * span, (n + 1) * span
            if backwards:
                shifted[lo:hi - rows, :] = h_ref[lo + rows:hi, :]
                shifted[hi - rows:hi, :] = none
            else:
                shifted[lo + rows:hi, :] = h_ref[lo:hi - rows, :]
                shifted[lo:lo + rows, :] = none
        turn(shifted)

    out_ref[...] = jnp.dot(turned[...], dz_ref[...], preferred_element_type=F32)


def weight_grad(x_all, h_all, dz_all, backwards, steps, planes=None, plane=None, into=None):
    devs, span, hid = x_all.shape
    count = devs * span
    wide = dz_all.shape[2]
    width = 512
    flat = lambda a: a.reshape(count, a.shape[-1])
    args = [flat(x_all), flat(h_all), flat(dz_all)]
    whole = pl.BlockSpec((count, hid), lambda p, n: (0, 0), pipeline_mode=pl.Buffered(1))
    in_specs = [whole, whole, pl.BlockSpec((count, width), lambda p, n: (0, n))]
    aliases = {}
    if into is not None:
        args.append(into)
        in_specs.append(pl.BlockSpec(memory_space=pl.ANY))
        aliases = {3: 0}
    if planes is None:
        out = jax.ShapeDtypeStruct((2 * hid, wide), F32)
        out_spec = pl.BlockSpec((hid, width), lambda p, n: (p, n))
    else:
        out = jax.ShapeDtypeStruct((planes, 2 * hid, wide), F32)
        out_spec = pl.BlockSpec((None, hid, width), lambda p, n: (plane, p, n))
    return pl.pallas_call(
        functools.partial(dw_kernel, backwards, steps, span // steps),
        grid=(2, wide // width),
        out_shape=out,
        in_specs=in_specs,
        out_specs=out_spec,
        scratch_shapes=[pltpu.VMEM((count, hid), BF16), pltpu.VMEM((hid, count), BF16)],
        input_output_aliases=aliases,
        compiler_params=pltpu.CompilerParams(vmem_limit_bytes=VMEM_LIMIT,
                                             dimension_semantics=('arbitrary', 'arbitrary')),
        cost_estimate=pl.CostEstimate(flops=4 * count * hid * wide, bytes_accessed=90 << 20, transcendentals=0),
        name='dw',
    )(*args)


def gather(rows):
    return lax.all_gather(rows, DATA_AXIS, axis=0)


def step_grads(inputs, out_grad, w_fwd0, b_fwd0, w_rev0, b_rev0, w_upper, b_upper):
    batch, steps, hid = inputs.shape
    seq = lambda a: a.reshape(steps, batch, a.shape[-1])
    row = lambda b: b[None, :]
    x_rows = jnp.swapaxes(inputs, 0, 1).reshape(steps * batch, hid)
    head, tail, last = {'start': (0,), 4: (1,)}, {'start': (2,)}, {'start': (3,)}
    gate_f, cprev_f, h_f, hb_f, all_x = lstm_forward(
        x_rows, w_fwd0, None, row(b_fwd0), steps, False, 0, gathers=(('x', None, head),))
    gate_r, cprev_r, h_r, hb_r, x1, all_x, all_f = lstm_forward(
        x_rows, w_rev0, None, row(b_rev0), steps, True, 1, h_f, gathers=(('alias', all_x, tail), ('arg', hb_f, head)))
    gate_1, cprev_1, _, hb_1, all_x, all_f, all_r, all_x1 = lstm_forward(
        x1, w_upper, 0, row(b_upper[0]), steps, False, 2,
        gathers=(('alias', all_x, last), ('alias', all_f, tail), ('arg', hb_r, head), ('x', None, head)))
    gate_2, cprev_2, _, hb_2, all_f, all_r, all_x1, all_1 = lstm_forward(
        hb_1, w_upper, 1, row(b_upper[1]), steps, False, 3,
        gathers=(('alias', all_f, last), ('alias', all_r, tail), ('alias', all_x1, tail), ('x', None, head)))

    dz_2, db_2, dx_2, all_r, all_x1, all_1, all_2 = lstm_backward(
        jnp.swapaxes(out_grad, 0, 1), w_upper, 1, gate_2, cprev_2, False, 4,
        gathers=(('alias', all_r, last), ('alias', all_x1, last), ('alias', all_1, tail),
                 ('arg', hb_2, {'start': (0,), 2: (1,), 5: (2,)})))
    dz_1, db_1, dx_1, all_1, all_2, dz2_all = lstm_backward(
        seq(dx_2), w_upper, 0, gate_1, cprev_1, False, 5,
        gathers=(('alias', all_1, last), ('alias', all_2, last), ('arg', dz_2, {'start': (0,), 3: (1,)})))
    dz_f, db_f, dx_f, dz2_all, dz1_all = lstm_backward(
        seq(dx_1), w_fwd0, None, gate_f, cprev_f, False, 6,
        gathers=(('alias', dz2_all, {'start': (2,)}), ('arg', dz_1, {'start': (0,), 5: (1,)})))
    dzf_all = gather(dz_f)
    dz_r, db_r, in_rows, dz2_all, dz1_all = lstm_backward(
        seq(dx_1), w_rev0, None, gate_r, cprev_r, True, 7, dx_f,
        gathers=(('alias', dz2_all, last), ('alias', dz1_all, {'start': (2,), 'end': (3,)})))
    dzr_all = gather(dz_r)
    in_grad = jnp.swapaxes(seq(in_rows), 0, 1)

    db_own = jnp.stack([jnp.sum(d, axis=0) for d in (db_1, db_2, db_f, db_r)])
    db_own, dzr_all = lax.optimization_barrier((db_own, dzr_all))
    db_all = jnp.sum(gather(db_own), axis=0)

    dw_up = weight_grad(all_1, all_2, dz2_all, False, steps, 2, 1)
    dw_up = weight_grad(all_x1, all_1, dz1_all, False, steps, 2, 0, dw_up)
    dw_f = weight_grad(all_x, all_f, dzf_all, False, steps)
    dw_r = weight_grad(all_x, all_r, dzr_all, True, steps)
    return (in_grad, dw_f, db_all[2], dw_r, db_all[3], dw_up, db_all[:2])


def solution(mesh):
    return jax.shard_map(step_grads, mesh=mesh,
                         in_specs=(P(DATA_AXIS), P(DATA_AXIS), P(), P(), P(), P(), P(), P()),
                         out_specs=(P(DATA_AXIS), P(), P(), P(), P(), P(), P()),
                         check_vma=False)
```

```python
import functools

import jax
import jax.numpy as jnp
from jax import lax
from jax.experimental import pallas as pl
from jax.experimental.pallas import tpu as pltpu
from jax.sharding import PartitionSpec as P

DATA_AXIS = 'data'
F32 = jnp.float32
BF16 = jnp.bfloat16
VMEM_LIMIT = 60 * 1024 * 1024


def dot_nt(lhs, rhs):
    return lax.dot_general(lhs, rhs, (((1,), (1,)), ((), ())), preferred_element_type=F32)


class Exchange:
    def __init__(self, ref, sems, fine):
        self.ref, self.sems, self.fine = ref, sems, fine
        self.third = ref.shape[-1] // 3
        self.me = lax.axis_index(DATA_AXIS)
        self.coord = {bit: (self.me // bit) % 2 for bit in (8, 4, 2, 1)}

    def peer(self, bit):
        return self.me + bit * (1 - 2 * self.coord[bit])

    def bits(self, part):
        return [2 << ((part + r) % 3) for r in range(3)]

    def view(self, at, part=None):
        index = tuple(pl.ds(0, 2) if at[bit] is None else at[bit] for bit in (8, 4, 2))
        cols = pl.ds(0, 3 * self.third) if part is None else pl.ds(part * self.third, self.third)
        return self.ref.at[index + (self.coord[1], slice(None), cols)]

    def copies(self, part, rnd):
        bits = self.bits(part)
        free = bits[:rnd]
        picks = [(None,) * rnd]
        if self.fine and rnd == 2:
            picks = [(0, 0), (0, 1), (1, 0), (1, 1)]
        out = []
        for j, pick in enumerate(picks):
            sent = dict(self.coord)
            sent.update(zip(free, pick))
            got = dict(sent)
            got[bits[rnd]] = 1 - sent[bits[rnd]]
            slot = part + 3 * rnd if rnd < 2 else 6 + 4 * part + j
            out.append((self.view(sent, part), self.view(got, part), self.peer(bits[rnd]), slot))
        return out

    def remote(self, view, peer, slot):
        return pltpu.make_async_remote_copy(
            src_ref=view, dst_ref=view, send_sem=self.sems.at[0, slot], recv_sem=self.sems.at[1, slot],
            device_id=(peer,), device_id_type=pl.DeviceIdType.MESH)

    def each(self, rnd):
        for copies in zip(*[self.copies(part, rnd) for part in range(3)]):
            yield from copies

    def send(self, rnd):
        for sent, got, peer, slot in self.each(rnd):
            self.remote(sent, peer, slot).start()

    def wait(self, rnd):
        for sent, got, peer, slot in self.each(rnd):
            self.remote(sent, peer, slot).wait()

    def own(self):
        return self.remote(self.view(self.coord), self.peer(1), 18)

    def share(self, rnd, start, arrived=True):
        for sent, got, peer, slot in self.each(rnd):
            if not arrived:
                self.remote(sent, peer, slot).wait()
            copy = self.remote(got, self.peer(1), 19 + slot)
            if start:
                copy.start()
            else:
                copy.wait()


SLOTS = 37


def run_stage(ex, stage, open_ops):
    arrived = True
    if stage > 0:
        if ('round', stage - 1) in open_ops:
            open_ops.remove(('round', stage - 1))
            arrived = stage < 3
            if arrived:
                ex.wait(stage - 1)
    else:
        ex.own().start()
        open_ops.append(('own', 0))
    if stage < 3:
        ex.send(stage)
        open_ops.append(('round', stage))
    if stage > 0:
        ex.share(stage - 1, True, arrived)
        open_ops.append(('share', stage - 1))


class Comm:
    def __init__(self, plan, refs, sems, local_sems, sources):
        self.plan = plan
        self.exs = [Exchange(ref, sems.at[n], 'fine' in p) for n, (ref, p) in enumerate(zip(refs, plan))]
        self.open_ops = [[] for _ in plan]
        self.local = [None if src is None else pltpu.make_async_copy(src, ex.view(ex.coord), local_sems.at[n])
                      for n, (src, ex) in enumerate(zip(sources, self.exs))]

    def begin(self):
        if not self.plan:
            return
        for copy in self.local:
            if copy is not None:
                copy.start()
        barrier = pltpu.get_barrier_semaphore()
        ex = self.exs[0]
        for bit in (1, 2, 4, 8):
            pl.semaphore_signal(barrier, inc=1, device_id=(ex.peer(bit),), device_id_type=pl.DeviceIdType.MESH)
        pl.semaphore_wait(barrier, 4)
        for copy in self.local:
            if copy is not None:
                copy.wait()
        self.at('start')

    def at(self, point):
        for ex, plan, ops in zip(self.exs, self.plan, self.open_ops):
            for stage in plan.get(point, ()):
                run_stage(ex, stage, ops)

    def in_loop(self, idx):
        points = sorted({p for plan in self.plan for p in plan if isinstance(p, int)})
        for point in points:
            pl.when(idx == point)(functools.partial(self.at, point))

    def finish(self):
        self.at('end')
        for ex, ops in zip(self.exs, self.open_ops):
            for kind, rnd in ops:
                if kind == 'round':
                    ex.wait(rnd)
                elif kind == 'share':
                    ex.share(rnd, False)
                else:
                    ex.own().wait()


def fwd_kernel(layer, bias_row, steps, backwards, with_sum, plan, sources, *refs):
    refs = list(refs)
    x_ref, w_hbm, b_ref = refs[:3]
    refs = refs[3:]
    other_ref = refs.pop(0) if with_sum else None
    srcs = [x_ref if s == 'x' else refs.pop(0) if s == 'arg' else None for s in sources]
    refs = refs[sum(s == 'alias' for s in sources):]
    gate_ref, cprev_ref, h_ref, hbf_ref = refs[:4]
    refs = refs[4:]
    sum_ref = refs.pop(0) if with_sum else None
    g_refs = [refs.pop(0) for _ in plan]
    w_buf, pre, sems = refs[:3]
    comm = Comm(plan, g_refs, *(refs[3:5] if plan else (None, None)), srcs)
    hid = x_ref.shape[1]
    rows = x_ref.shape[0] // steps
    w_src = w_hbm if layer is None else w_hbm.at[layer]

    def w_copy(part, gate):
        at = (pl.ds(part * hid, hid), pl.ds(gate * hid, hid))
        return pltpu.make_async_copy(w_src.at[at], w_buf.at[at], sems.at[part * 4 + gate])

    for part in range(2):
        for gate in range(4):
            w_copy(part, gate).start()
    comm.begin()
    for gate in range(4):
        w_copy(0, gate).wait()
        cols = pl.ds(gate * hid, hid)
        pre[:, cols] = jnp.dot(x_ref[...], w_buf[:hid, cols], preferred_element_type=F32) + b_ref[bias_row:bias_row + 1, cols]

    def cell(t, z_all, c_prev):
        in_gate = jax.nn.sigmoid(z_all[:, :hid])
        forget_gate = jax.nn.sigmoid(z_all[:, hid:2 * hid])
        cand_gate = jnp.tanh(z_all[:, 2 * hid:3 * hid])
        out_gate = jax.nn.sigmoid(z_all[:, 3 * hid:])
        c_new = forget_gate * c_prev + in_gate * cand_gate
        h_new = out_gate * jnp.tanh(c_new)
        gate_ref[t, :, :hid] = in_gate
        gate_ref[t, :, hid:2 * hid] = forget_gate
        gate_ref[t, :, 2 * hid:3 * hid] = cand_gate
        gate_ref[t, :, 3 * hid:] = out_gate
        cprev_ref[t] = c_prev
        h_ref[t] = h_new
        h_bf = h_new.astype(BF16)
        at = pl.ds(t * rows, rows) if isinstance(t, int) else pl.ds(pl.multiple_of(t * rows, rows), rows)
        hbf_ref[at, :] = h_bf
        if with_sum:
            sum_ref[at, :] = (other_ref[t] + h_new).astype(BF16)
        return h_bf, c_new

    first = steps - 1 if backwards else 0
    carry = cell(first, pre[first * rows:(first + 1) * rows, :], jnp.zeros((rows, hid), F32))
    for gate in range(4):
        w_copy(1, gate).wait()

    def step(idx, carry):
        h_bf, c_prev = carry
        comm.in_loop(idx)
        t = steps - 1 - idx if backwards else idx
        z_all = pre[pl.ds(pl.multiple_of(t * rows, rows), rows), :] + jnp.dot(
            h_bf, w_buf[hid:, :], preferred_element_type=F32)
        return cell(t, z_all, c_prev)

    lax.fori_loop(1, steps, step, carry)
    comm.finish()


def call(kernel, name, args, n_vmem, outs, scratch, plan, blocks, aliases, collective, flops):
    vm, hbm = pl.BlockSpec(memory_space=pltpu.VMEM), pl.BlockSpec(memory_space=pl.ANY)
    in_specs = [hbm if n == 1 or n >= n_vmem else vm for n in range(len(args))]
    out_specs = [vm] * len(outs) + [hbm] * len(blocks)
    params = dict(vmem_limit_bytes=VMEM_LIMIT)
    if plan:
        params.update(collective_id=collective, has_side_effects=True)
        scratch = scratch + [pltpu.SemaphoreType.DMA((len(plan), 2, SLOTS)), pltpu.SemaphoreType.DMA((len(plan),))]
    return pl.pallas_call(
        kernel,
        out_shape=outs + [jax.ShapeDtypeStruct(shape, BF16) for shape in blocks],
        in_specs=in_specs,
        out_specs=out_specs,
        scratch_shapes=scratch,
        input_output_aliases=aliases,
        compiler_params=pltpu.CompilerParams(**params),
        cost_estimate=pl.CostEstimate(flops=flops, bytes_accessed=40 << 20, transcendentals=0),
        name=name,
    )(*args)


def gather_args(args, gathers, n_outs, x_rows):
    args += [blk for kind, blk, _ in gathers if kind == 'arg']
    n_vmem = len(args)
    aliases = {}
    blocks = []
    for n, (kind, blk, _) in enumerate(gathers):
        if kind == 'alias':
            aliases[len(args)] = n_outs + n
            args.append(blk)
            blocks.append(blk.shape)
        else:
            blocks.append((2, 2, 2, 2) + (x_rows if kind == 'x' else blk).shape)
    return [p for _, _, p in gathers], [kind for kind, _, _ in gathers], blocks, n_vmem, aliases


def lstm_forward(x_rows, w_cat, layer, biases, bias_row, steps, backwards, collective, other=None, gathers=()):
    hid = x_rows.shape[1]
    rows = x_rows.shape[0] // steps
    with_sum = other is not None
    outs = [jax.ShapeDtypeStruct((steps, rows, 4 * hid), F32),
            jax.ShapeDtypeStruct((steps, rows, hid), F32),
            jax.ShapeDtypeStruct((steps, rows, hid), F32),
            jax.ShapeDtypeStruct((steps * rows, hid), BF16)]
    args = [x_rows, w_cat, biases]
    if with_sum:
        outs.append(jax.ShapeDtypeStruct((steps * rows, hid), BF16))
        args.append(other)
    plan, sources, blocks, n_vmem, aliases = gather_args(args, gathers, len(outs), x_rows)
    return call(functools.partial(fwd_kernel, layer, bias_row, steps, backwards, with_sum, plan, sources), 'lstm_fwd', args,
                n_vmem, outs,
                [pltpu.VMEM((2 * hid, 4 * hid), BF16), pltpu.VMEM((steps * rows, 4 * hid), F32),
                 pltpu.SemaphoreType.DMA((8,))],
                plan, blocks, aliases, collective, 4 * steps * rows * hid * 4 * hid * 8)


def bwd_kernel(layer, steps, backwards, with_sum, plan, sources, *refs):
    refs = list(refs)
    dh_ref, w_hbm, gate_ref, cprev_ref = refs[:4]
    refs = refs[4:]
    other_ref = refs.pop(0) if with_sum else None
    srcs = [refs.pop(0) if s == 'arg' else None for s in sources]
    refs = refs[sum(s == 'alias' for s in sources):]
    dz_ref, db_ref, dx_ref = refs[:3]
    refs = refs[3:]
    g_refs = [refs.pop(0) for _ in plan]
    w_buf, sems = refs[:2]
    comm = Comm(plan, g_refs, *(refs[2:4] if plan else (None, None)), srcs)
    rows, hid = dh_ref.shape[1:]
    w_src = w_hbm if layer is None else w_hbm.at[layer]

    def w_copy(part):
        at = pl.ds(part * hid, hid)
        return pltpu.make_async_copy(w_src.at[at], w_buf.at[at], sems.at[part])

    w_copy(1).start()
    w_copy(0).start()
    comm.begin()

    def cell(t, dh_rec, dc_next):
        in_gate = gate_ref[t, :, :hid]
        forget_gate = gate_ref[t, :, hid:2 * hid]
        cand_gate = gate_ref[t, :, 2 * hid:3 * hid]
        out_gate = gate_ref[t, :, 3 * hid:]
        c_prev = cprev_ref[t]
        tanh_c = jnp.tanh(forget_gate * c_prev + in_gate * cand_gate)
        dh_tot = dh_ref[t] + dh_rec
        dc_cur = dc_next + dh_tot * out_gate * (1.0 - tanh_c * tanh_c)
        parts = [dc_cur * cand_gate * in_gate * (1.0 - in_gate),
                 dc_cur * c_prev * forget_gate * (1.0 - forget_gate),
                 dc_cur * in_gate * (1.0 - cand_gate * cand_gate),
                 dh_tot * tanh_c * out_gate * (1.0 - out_gate)]
        at = pl.ds(pl.multiple_of(t * rows, rows), rows)
        for gate, part in enumerate(parts):
            cols = slice(gate * hid, (gate + 1) * hid)
            dz_ref[at, cols] = part.astype(BF16)
            db_ref[:, cols] += part[:8] + part[8:]
        return dc_cur * forget_gate

    db_ref[...] = jnp.zeros_like(db_ref)
    first = 0 if backwards else steps - 1
    zero = jnp.zeros((rows, hid), F32)
    dc = cell(first, zero, zero)
    w_copy(1).wait()

    def step(idx, dc_next):
        comm.in_loop(idx)
        prev = idx - 1 if backwards else steps - idx
        t = idx if backwards else steps - 1 - idx
        at = pl.ds(pl.multiple_of(prev * rows, rows), rows)
        dh_rec = dot_nt(dz_ref[at, :], w_buf[hid:, :])
        return cell(t, dh_rec, dc_next)

    lax.fori_loop(1, steps, step, dc)
    w_copy(0).wait()
    dx = dot_nt(dz_ref[...], w_buf[:hid, :])
    if with_sum:
        dx = dx + other_ref[...]
    dx_ref[...] = dx
    comm.finish()


def lstm_backward(dh_seq, w_cat, layer, gate_seq, c_prevs, backwards, collective, other=None, gathers=()):
    steps, rows, hid = dh_seq.shape
    with_sum = other is not None
    args = [dh_seq, w_cat, gate_seq, c_prevs] + ([other] if with_sum else [])
    plan, sources, blocks, n_vmem, aliases = gather_args(args, gathers, 3, None)
    return call(functools.partial(bwd_kernel, layer, steps, backwards, with_sum, plan, sources), 'lstm_bwd', args,
                n_vmem,
                [jax.ShapeDtypeStruct((steps * rows, 4 * hid), BF16),
                 jax.ShapeDtypeStruct((8, 4 * hid), F32),
                 jax.ShapeDtypeStruct((steps * rows, hid), F32)],
                [pltpu.VMEM((2 * hid, 4 * hid), BF16), pltpu.SemaphoreType.DMA((2,))],
                plan, blocks, aliases, collective, 4 * steps * rows * hid * 4 * hid * 12)


def dw_kernel(backwards, steps, rows, x_hbm, h_hbm, dz_ref, *refs):
    out_ref, x_buf, h_buf, x_turned, h_turned, x_sems, h_sems = refs[-7:]
    part, col = pl.program_id(0), pl.program_id(1)
    span = steps * rows
    devs = x_buf.shape[0] // span

    def copy(src, dst, sems, n):
        at = pl.ds(pl.multiple_of(n * span, span), span)
        return pltpu.make_async_copy(src.at[at], dst.at[at], sems.at[n])

    @pl.when((part == 0) & (col == 0))
    def _():
        for n in range(devs):
            copy(x_hbm, x_buf, x_sems, n).start()
        for n in range(devs):
            copy(h_hbm, h_buf, h_sems, n).start()
        for n in range(devs):
            copy(x_hbm, x_buf, x_sems, n).wait()
            x_turned[:, n * span:(n + 1) * span] = x_buf[n * span:(n + 1) * span, :].T

    @pl.when((part == 0) & (col < devs // 2))
    def _():
        for half in range(2):
            copy(h_hbm, h_buf, h_sems, 2 * col + half).wait()

    @pl.when(part == 0)
    def _():
        none = jnp.zeros((rows, h_buf.shape[1]), BF16)
        for half in range(2):
            first = pl.multiple_of((2 * jnp.minimum(col, devs // 2 - 1) + half) * span, span)
            if backwards:
                prev = jnp.concatenate([h_buf[pl.ds(first + rows, span - rows), :], none], axis=0)
            else:
                prev = jnp.concatenate([none, h_buf[pl.ds(first, span - rows), :]], axis=0)
            h_turned[:, pl.ds(first, span)] = prev.T
        out_ref[...] = jnp.dot(x_turned[...], dz_ref[...], preferred_element_type=F32)

    @pl.when(part == 1)
    def _():
        out_ref[...] = jnp.dot(h_turned[...], dz_ref[...], preferred_element_type=F32)


def weight_grad(x_all, h_all, dz_all, backwards, steps, planes=None, plane=None, into=None):
    span, hid = x_all.shape[-2:]
    count = x_all.size // hid
    devs = count // span
    wide = dz_all.shape[-1]
    width = 512
    flat = lambda a: a.reshape(count, a.shape[-1])
    args = [flat(x_all), flat(h_all), flat(dz_all)]
    hbm = pl.BlockSpec(memory_space=pl.ANY)
    in_specs = [hbm, hbm, pl.BlockSpec((count, width), lambda p, n: (0, n))]
    aliases = {}
    if into is not None:
        args.append(into)
        in_specs.append(hbm)
        aliases = {3: 0}
    if planes is None:
        out = jax.ShapeDtypeStruct((2 * hid, wide), F32)
        out_spec = pl.BlockSpec((hid, width), lambda p, n: (p, n))
    else:
        out = jax.ShapeDtypeStruct((planes, 2 * hid, wide), F32)
        out_spec = pl.BlockSpec((None, hid, width), lambda p, n: (plane, p, n))
    return pl.pallas_call(
        functools.partial(dw_kernel, backwards, steps, span // steps),
        grid=(2, wide // width),
        out_shape=out,
        in_specs=in_specs,
        out_specs=out_spec,
        scratch_shapes=[pltpu.VMEM((count, hid), BF16)] * 2 + [pltpu.VMEM((hid, count), BF16)] * 2
        + [pltpu.SemaphoreType.DMA((devs,))] * 2,
        input_output_aliases=aliases,
        compiler_params=pltpu.CompilerParams(vmem_limit_bytes=VMEM_LIMIT,
                                             dimension_semantics=('arbitrary', 'arbitrary')),
        cost_estimate=pl.CostEstimate(flops=4 * count * hid * wide, bytes_accessed=90 << 20, transcendentals=0),
        name='dw',
    )(*args)


def gather(rows):
    return lax.all_gather(rows, DATA_AXIS, axis=0)


def step_grads(inputs, out_grad, w_fwd0, b_fwd0, w_rev0, b_rev0, w_upper, b_upper):
    batch, steps, hid = inputs.shape
    seq = lambda a: a.reshape(steps, batch, a.shape[-1])
    x_rows = jnp.swapaxes(inputs, 0, 1).reshape(steps * batch, hid)
    head, tail, last = {'start': (0,), 1: (1,)}, {'start': (2,)}, {'start': (3,)}
    late = {'start': (0,), 2: (1,)}
    b_low = jnp.stack([b_fwd0, b_rev0])
    gate_f, cprev_f, h_f, hb_f, all_x = lstm_forward(
        x_rows, w_fwd0, None, b_low, 0, steps, False, 0, gathers=(('x', None, head),))
    gate_r, cprev_r, h_r, hb_r, x1, all_f, all_x = lstm_forward(
        x_rows, w_rev0, None, b_low, 1, steps, True, 1, h_f, gathers=(('arg', hb_f, head), ('alias', all_x, tail)))
    gate_1, cprev_1, _, hb_1, all_r, all_x1, all_f, all_x = lstm_forward(
        x1, w_upper, 0, b_upper, 0, steps, False, 2,
        gathers=(('arg', hb_r, late), ('x', None, late), ('alias', all_f, tail), ('alias', all_x, last)))
    gate_2, cprev_2, _, hb_2, all_1, all_r, all_x1, all_f = lstm_forward(
        hb_1, w_upper, 1, b_upper, 1, steps, False, 3,
        gathers=(('x', None, {'start': (0,)}), ('alias', all_r, tail), ('alias', all_x1, tail),
                 ('alias', all_f, last)))

    dz_2, db_2, dx_2, all_2, all_1, all_r, all_x1 = lstm_backward(
        jnp.swapaxes(out_grad, 0, 1), w_upper, 1, gate_2, cprev_2, False, 4,
        gathers=(('arg', hb_2, {'start': (0,), 2: (1,), 5: (2,)}), ('alias', all_1, {'start': (1,), 2: (2,)}),
                 ('alias', all_r, last), ('alias', all_x1, last)))
    dz_1, db_1, dx_1, dz2_all, all_2, all_1 = lstm_backward(
        seq(dx_2), w_upper, 0, gate_1, cprev_1, False, 5,
        gathers=(('arg', dz_2, {'start': (0,), 3: (1,)}), ('alias', all_2, last), ('alias', all_1, last)))
    dz_f, db_f, dx_f, dz1_all, dz2_all = lstm_backward(
        seq(dx_1), w_fwd0, None, gate_f, cprev_f, False, 6,
        gathers=(('arg', dz_1, {'start': (0,), 4: (1,)}), ('alias', dz2_all, tail)))
    dzf_all = gather(dz_f)
    dz_r, db_r, in_rows, dz1_all, dz2_all = lstm_backward(
        seq(dx_1), w_rev0, None, gate_r, cprev_r, True, 7, dx_f,
        gathers=(('alias', dz1_all, {'fine': (), 'start': (2,), 'end': (3,)}), ('alias', dz2_all, last)))
    dzr_all = gather(dz_r)
    in_grad = jnp.swapaxes(seq(in_rows), 0, 1)

    db_own = jnp.stack([jnp.sum(d, axis=0) for d in (db_1, db_2, db_f, db_r)])
    db_own, dzr_all = lax.optimization_barrier((db_own, dzr_all))
    db_all = jnp.sum(gather(db_own), axis=0)

    dw_up = weight_grad(all_1, all_2, dz2_all, False, steps, 2, 1)
    dw_up = weight_grad(all_x1, all_1, dz1_all, False, steps, 2, 0, dw_up)
    dw_f = weight_grad(all_x, all_f, dzf_all, False, steps)
    dw_r = weight_grad(all_x, all_r, dzr_all, True, steps)
    return (in_grad, dw_f, db_all[2], dw_r, db_all[3], dw_up, db_all[:2])


def solution(mesh):
    return jax.shard_map(step_grads, mesh=mesh,
                         in_specs=(P(DATA_AXIS), P(DATA_AXIS), P(), P(), P(), P(), P(), P()),
                         out_specs=(P(DATA_AXIS), P(), P(), P(), P(), P(), P()),
                         check_vma=False)
```
